32 devices in a mesh: rows: 32 (over z, y, x, core).
Axes of the slice: x: 2, y: 2, z: 4, core: 2. Of those that a mesh axis runs over, the one named last changes fastest.
Arguments:
- edge_tiles: bfloat16 [8192, 128, 128], P('rows'), may hold values from -0.5 to 0.5
- tile_row: int32 [8192], P('rows'), may hold values from 0 to 7
- tile_slot: int32 [8192], P('rows'), may hold values from 0 to 63, as said below
- tile_count: int32 [32], P('rows'), may hold values from 32 to 256, as said below
- fetch_list: int32 [32, 64], P('rows'), may hold values from 0 to 7, as said below
- hub_start: float32 [8, 32768], P(None, 'rows'), may hold values from -6 to 6
Outputs:
- hub: float32 [8, 32768], P(None, 'rows')
- authority: float32 [8, 32768], P(None, 'rows')
The draws below stay inside these ranges and needn't reach their ends.
Inputs may be any that keep to these rules, and one draw needn't show every extreme that they name: tile_slot[t] = p * 2 + k names entry k of the fetch_list group of device p, in the row of the tile's own device. `fetch_list`: entries p * 2 to p * 2 + 1 of each row are 2 distinct block numbers among device p's own 8 blocks. Tile slots of device d at positions 256 * d + i with i >= tile_count[d] are not part of the graph.
All inputs are finite; a program needn't handle non-finite values.
Results may differ from the reference program's by a relative error of at most 0.004.
Values may be sent and summed in bfloat16 or wider, within the bound.
No kernel may reach another device: no remote copies, remote signals or barrier semaphores. Data moves between devices by JAX's collectives and lax.ppermute only.
A program may use at most 64 MiB of HBM per device.

```python
import jax
import jax.numpy as jnp
from jax import lax

TILE = 128
COLS = 8
BLK_DEV = 8
TILES_DEV = 256
SLOTS = 2
ITERS = 2
NODES = 32768
TILES = 8192
N_ROWS = 32


def draw_tile_slot(key, part):
    owner_ids = jnp.arange(N_ROWS, dtype=jnp.int32)
    weights = N_ROWS + 3 * owner_ids
    cumulative = jnp.cumsum(weights).astype(jnp.int32)
    key_owner, key_entry = jax.random.split(jax.random.fold_in(key, 11))
    picks = jax.random.randint(key_owner, (TILES_DEV * N_ROWS,), 0, cumulative[N_ROWS - 1], dtype=jnp.int32)
    owners = jnp.searchsorted(cumulative, picks, side='right').astype(jnp.int32)
    entries = jax.random.randint(key_entry, (TILES_DEV * N_ROWS,), 0, SLOTS, dtype=jnp.int32)
    return (owners * SLOTS + entries).astype(jnp.int32)


def draw_tile_count(key, part):
    position = jnp.arange(N_ROWS, dtype=jnp.int32)
    lowest = TILES_DEV // 8
    extent = TILES_DEV - lowest
    divisor = max(N_ROWS - 1, 1)
    rising = lowest + extent * position * position // (divisor * divisor)
    jitter_term = jax.random.randint(jax.random.fold_in(key, 23), (N_ROWS,), -(TILES_DEV // 16), TILES_DEV // 16 + 1, dtype=jnp.int32)
    counted = jnp.clip(rising + jitter_term, lowest, TILES_DEV)
    return counted.at[N_ROWS - 1].set(TILES_DEV).astype(jnp.int32)


def draw_fetch_list(key, part):
    scores = jax.random.randint(jax.random.fold_in(key, 37), (N_ROWS, N_ROWS, BLK_DEV), 0, 1 << 20, dtype=jnp.int32)
    ordering = jnp.argsort(scores, axis=-1, stable=True)[:, :, :SLOTS]
    return ordering.reshape(N_ROWS, N_ROWS * SLOTS).astype(jnp.int32)


def place_ends(values, own_key, least, high):
    longest = values.shape.index(max(values.shape))
    spots = []
    for shift in (0, 1):
        where = [jax.random.randint(jax.random.fold_in(own_key, axis), (), 0, length) for axis, length in enumerate(values.shape)]
        where[longest] = (where[longest] + shift) % values.shape[longest]
        spots.append(tuple(where))
    return values.at[spots[0]].set(least).at[spots[1]].set(high)


def block_scale(key, dims, shards, least, high):
    factor_of = 1.0
    for axis_at, shards_of in shards:
        heights = jax.random.uniform(jax.random.fold_in(jax.random.fold_in(key, 6), axis_at), (shards_of,), jnp.float32, least / len(shards), high / len(shards))
        factor_of = factor_of * jnp.repeat(jnp.exp(heights), dims[axis_at] // shards_of).reshape((-1,) + (1,) * (len(dims) - 1 - axis_at))
    return factor_of


def scatter_about(rng, shape, width, most, cuts=(), kind=jnp.bfloat16):
    gain = block_scale(rng, shape, cuts, -0.22, 0.18) if cuts else 1.0
    array = jax.random.normal(rng, shape, jnp.float32) * width * gain
    return jnp.minimum(jnp.maximum(array, -most), most).astype(kind)


def setup_inputs(seed: int = 0) -> dict:
    keys = jax.random.split(jax.random.key(seed), 7)
    return {
        "edge_tiles": scatter_about(keys[0], (TILES, TILE, TILE), TILE ** -0.5, 0.5, ((0, 32),)),
        "tile_row": place_ends(jax.random.randint(keys[1], (TILES,), 0, BLK_DEV), jax.random.fold_in(keys[1], 1), 0, BLK_DEV - 1).astype(jnp.int32),
        "tile_slot": draw_tile_slot(jax.random.fold_in(keys[6], 71), 0),
        "tile_count": draw_tile_count(jax.random.fold_in(keys[6], 71), 0),
        "fetch_list": draw_fetch_list(jax.random.fold_in(keys[6], 71), 0),
        "hub_start": scatter_about(keys[5], (COLS, NODES), 1.0, 6.0, ((1, 32),), jnp.float32),
    }


def column_scale(raw_blocks):
    mean_square = lax.optimization_barrier(jnp.sum(raw_blocks * raw_blocks, axis=(0, 2))) / (BLK_DEV * N_ROWS * TILE)
    return raw_blocks / jnp.sqrt(mean_square + 1e-06)[None, :, None]

def reference(edge_tiles, tile_row, tile_slot, tile_count, fetch_list, hub_start):
    blocks = BLK_DEV * N_ROWS
    tiles_split = edge_tiles.reshape(N_ROWS, TILES_DEV, TILE, TILE)
    rows_split = tile_row.reshape(N_ROWS, TILES_DEV).astype(jnp.int32)
    slots_split = tile_slot.reshape(N_ROWS, TILES_DEV).astype(jnp.int32)
    device_ids = jnp.arange(N_ROWS, dtype=jnp.int32)

    def placement(rows_here, slots_here, count_here, fetch_here, device):
        rows_global = device * BLK_DEV + rows_here
        owners = slots_here // SLOTS
        cols_global = owners * BLK_DEV + jnp.take(fetch_here, slots_here).astype(jnp.int32)
        alive_mask = (jnp.arange(TILES_DEV, dtype=jnp.int32) < count_here).astype(jnp.float32)
        return (rows_global, cols_global, alive_mask)

    def transpose_pass(hub_low):

        def per_device(running, inputs):
            tiles_here, rows_here, slots_here, count_here, fetch_here, device = inputs
            rows_global, cols_global, alive_mask = placement(rows_here, slots_here, count_here, fetch_here, device)
            source = jnp.take(hub_low, rows_global, axis=0).astype(jnp.float32)
            product = jnp.einsum('gce,gef->gcf', source, tiles_here.astype(jnp.float32), precision=lax.Precision.HIGHEST)
            product = product * alive_mask[:, None, None]
            return (running + jax.ops.segment_sum(product, cols_global, num_segments=blocks), None)
        start_value = jnp.zeros((blocks, COLS, TILE), jnp.float32)
        running, _ = lax.scan(per_device, start_value, (tiles_split, rows_split, slots_split, tile_count.astype(jnp.int32), fetch_list.astype(jnp.int32), device_ids))
        return running

    def forward_pass(authority_low):

        def per_device(running, inputs):
            tiles_here, rows_here, slots_here, count_here, fetch_here, device = inputs
            rows_global, cols_global, alive_mask = placement(rows_here, slots_here, count_here, fetch_here, device)
            source = jnp.take(authority_low, cols_global, axis=0).astype(jnp.float32)
            product = jnp.einsum('gcf,gef->gce', source, tiles_here.astype(jnp.float32), precision=lax.Precision.HIGHEST)
            product = product * alive_mask[:, None, None]
            return (running + jax.ops.segment_sum(product, rows_global, num_segments=blocks), None)
        start_value = jnp.zeros((blocks, COLS, TILE), jnp.float32)
        running, _ = lax.scan(per_device, start_value, (tiles_split, rows_split, slots_split, tile_count.astype(jnp.int32), fetch_list.astype(jnp.int32), device_ids))
        return running
    hub_blocks = hub_start.reshape(COLS, blocks, TILE).transpose(1, 0, 2)
    hub_low = hub_blocks.astype(jnp.bfloat16)
    authority_blocks = hub_blocks
    for sweep in range(ITERS):
        authority_raw = transpose_pass(hub_low)
        authority_low = authority_raw.astype(jnp.bfloat16)
        hub_raw = forward_pass(authority_low)
        hub_blocks = column_scale(hub_raw)
        hub_low = hub_blocks.astype(jnp.bfloat16)
        authority_blocks = column_scale(authority_raw)
    hub = hub_blocks.transpose(1, 0, 2).reshape(COLS, blocks * TILE)
    authority = authority_blocks.transpose(1, 0, 2).reshape(COLS, blocks * TILE)
    return (hub, authority)
```

```python
import math

import jax
import jax.numpy as jnp
from jax import lax
from jax.experimental import pallas as pl
from jax.experimental.pallas import tpu as pltpu
from jax.sharding import PartitionSpec as P

ITERS = 2
EPS = 1e-06
GROUP = 8
CHUNK = 16
VMEM_LIMIT = 24 * 1024 * 1024

F32 = jnp.float32
BF16 = jnp.bfloat16


def tile_sweep(transposed, count, row_s, slot_s, tiles, source, accum, chunk, group, arrive):
    zero_at = source.shape[0] - 1
    columns, edge = source.shape[1:]
    half = group // 2
    pick, put = (row_s, slot_s) if transposed else (slot_s, row_s)

    def one_group(base):
        blocks = []
        targets = []
        for t in range(group):
            at = base + t
            blocks.append(source[jnp.where(at < count, pick[at], zero_at)])
            targets.append(put[at])
        pad = jnp.zeros((columns * half, edge), F32)
        left = jnp.concatenate(
            [
                jnp.concatenate(blocks[0::2] + [pad], 0),
                jnp.concatenate([pad] + blocks[1::2], 0),
            ],
            1,
        ).astype(BF16)
        weights = [tiles[base + t] for t in range(group)]
        outer, inner = (1, 0) if transposed else (0, 1)
        right = jnp.concatenate(
            [jnp.concatenate(weights[0::2], outer), jnp.concatenate(weights[1::2], outer)], inner
        )
        product = lax.dot_general(
            left, right, (((1,), (inner,)), ((), ())), preferred_element_type=F32
        )
        for t in range(group):
            first = (t % 2) * columns * half + (t // 2) * columns
            lane = (t // 2) * edge
            accum[targets[t]] += product[first : first + columns, lane : lane + edge]

    def one_chunk(c, carry):
        arrive(c)

        def two_groups(g, inner_carry):
            base = c * chunk + g * 2 * group
            one_group(base)
            one_group(base + group)
            return inner_carry

        return lax.fori_loop(0, chunk // (2 * group), two_groups, carry)

    lax.fori_loop(0, (count + chunk - 1) // chunk, one_chunk, 0)


def pack_blocks(accum, send, devices, slots_each):
    columns = accum.shape[1]
    for p in range(devices):
        both = jnp.concatenate([accum[p * slots_each + k] for k in range(slots_each)], 0)
        send[p, : slots_each * columns, :] = both.astype(BF16)


def solution(mesh):
    devices = mesh.shape["rows"]

    def per_device(edge_tiles, tile_row, tile_slot, tile_count, fetch_list, hub_start):
        tile_total, edge, _ = edge_tiles.shape
        columns = hub_start.shape[0]
        blocks = hub_start.shape[1] // edge
        slot_total = fetch_list.shape[1]
        slots_each = slot_total // devices
        node_total = hub_start.shape[1] * devices
        chunk = math.gcd(CHUNK, tile_total)
        group = min(GROUP, chunk // 2)
        rows_each = slots_each * columns
        assert blocks**slots_each <= 256 and group % 2 == 0

        smem = pl.BlockSpec(memory_space=pltpu.SMEM)
        vmem = pl.BlockSpec(memory_space=pltpu.VMEM)
        hbm = pl.BlockSpec(memory_space=pltpu.HBM)
        params = pltpu.CompilerParams(vmem_limit_bytes=VMEM_LIMIT)

        def start_kernel(cnt, row_s, slot_s, fetch, hub, tiles, send, kept, source, accum, sems):
            count = cnt[0]

            def copy(c):
                span = pl.ds(c * chunk, chunk)
                return pltpu.make_async_copy(tiles.at[span], kept.at[span], sems.at[c])

            def begin(c, carry):
                copy(c).start()
                return carry

            lax.fori_loop(0, (count + chunk - 1) // chunk, begin, 0)
            for b in range(blocks):
                source[b] = hub[:, b * edge : (b + 1) * edge].astype(BF16).astype(F32)
            source[blocks] = jnp.zeros((columns, edge), F32)
            accum[...] = jnp.zeros_like(accum)
            tile_sweep(
                True, count, row_s, slot_s, kept, source, accum, chunk, group,
                lambda c: copy(c).wait(),
            )
            pack_blocks(accum, send, devices, slots_each)
            for p in range(devices):
                code = fetch[0, p * slots_each]
                for k in range(1, slots_each):
                    code = code + fetch[0, p * slots_each + k] * blocks**k
                send[p, rows_each:, :] = jnp.full((columns, edge), code, jnp.int32).astype(F32).astype(BF16)

        def owner_kernel(got, codes, raw, reply, squares):
            totals = [jnp.zeros((columns, edge), F32) for _ in range(blocks)]

            def entries(p):
                code = codes[p, rows_each:, :].astype(F32)
                wanted = []
                for k in range(slots_each - 1, 0, -1):
                    high = jnp.floor(code * (1.0 / blocks**k))
                    wanted.append(high)
                    code = code - high * blocks**k
                return (wanted + [code])[::-1]

            for p in range(devices):
                wanted = entries(p)
                values = got[p, :rows_each, :].astype(F32)
                for k in range(slots_each):
                    value = values[k * columns : (k + 1) * columns]
                    for b in range(blocks):
                        totals[b] = totals[b] + jnp.where(wanted[k] == b, value, 0.0)
            square = jnp.zeros((columns, edge), F32)
            for b in range(blocks):
                raw[:, b * edge : (b + 1) * edge] = totals[b]
                square = square + totals[b] * totals[b]
            squares[...] = square
            for p in range(devices):
                wanted = entries(p)
                out = []
                for k in range(slots_each):
                    chosen = totals[0]
                    for b in range(1, blocks):
                        chosen = jnp.where(wanted[k] == b, totals[b], chosen)
                    out.append(chosen)
                reply[p] = jnp.concatenate(out, 0).astype(BF16)

        def load_fetched(fetched, source):
            for p in range(devices):
                both = fetched[p].astype(F32)
                for k in range(slots_each):
                    source[p * slots_each + k] = both[k * columns : (k + 1) * columns]
            source[slot_total] = jnp.zeros((columns, edge), F32)

        def middle_kernel(cnt, row_s, slot_s, fetched, tiles, send, squares, source, hub, accum, low):
            count = cnt[0]
            load_fetched(fetched, source)
            hub[...] = jnp.zeros_like(hub)
            accum[...] = jnp.zeros_like(accum)
            tile_sweep(
                False, count, row_s, slot_s, tiles, source, hub, chunk, group, lambda c: None
            )
            square = jnp.zeros((columns, edge), F32)
            for b in range(blocks):
                value = hub[b]
                square = square + value * value
                low[b] = value.astype(BF16).astype(F32)
            low[blocks] = jnp.zeros((columns, edge), F32)
            squares[...] = square
            tile_sweep(
                True, count, row_s, slot_s, tiles, low, accum, chunk, group, lambda c: None
            )
            pack_blocks(accum, send, devices, slots_each)

        def last_kernel(cnt, row_s, slot_s, fetched, tiles, first_squares, authority_squares, raw, send, source, hub):
            count = cnt[0]
            load_fetched(fetched, source)
            hub[...] = jnp.zeros_like(hub)
            tile_sweep(
                False, count, row_s, slot_s, tiles, source, hub, chunk, group, lambda c: None
            )
            largest = jnp.zeros((columns, edge), F32)
            for b in range(blocks):
                largest = jnp.maximum(largest, jnp.abs(hub[b]))
            peak = jnp.max(largest, axis=1, keepdims=True)
            inverse = jnp.where(peak > 1e-30, 1.0 / jnp.maximum(peak, 1e-30), 0.0)
            square = jnp.zeros((columns, edge), F32)
            for b in range(blocks):
                value = hub[b]
                raw[:, b * edge : (b + 1) * edge] = value
                scaled = value * inverse
                square = square + scaled * scaled
            stats = [
                jnp.sum(first_squares[...], axis=1, keepdims=True),
                jnp.sum(authority_squares[...], axis=1, keepdims=True),
                jnp.sum(square, axis=1, keepdims=True),
                peak,
            ]
            lane = lax.broadcasted_iota(jnp.int32, (columns, edge), 1)
            sub = lax.broadcasted_iota(jnp.int32, (columns, edge), 0)
            mixed = jnp.zeros((columns, edge), F32)
            for j, stat in enumerate(stats):
                mixed = jnp.where(lane == sub + j * columns, stat, mixed)
            line = jnp.sum(mixed, axis=0, keepdims=True)
            send[...] = jnp.broadcast_to(line, send.shape)

        def finish_kernel(got, hub_raw, authority_raw, hub, authority):
            rows = got[...]
            lane = lax.broadcasted_iota(jnp.int32, (columns, edge), 1)
            sub = lax.broadcasted_iota(jnp.int32, (columns, edge), 0)

            def column(line, j):
                spread = jnp.broadcast_to(line, (columns, edge))
                kept = jnp.where(lane == sub + j * columns, spread, 0.0)
                return jnp.sum(kept, axis=1, keepdims=True)

            sums = jnp.sum(rows, axis=0, keepdims=True)
            first = column(sums, 0) / node_total
            first_scale = 1.0 / jnp.sqrt(first + EPS)
            authority_mean = column(sums, 1) / node_total * first_scale * first_scale
            at_peaks = jnp.sum(
                jnp.where(lane == sub + 3 * columns, first_scale, 0.0), axis=0, keepdims=True
            )
            peaks = rows * at_peaks
            peaks = pltpu.roll(peaks, edge - columns, 1)
            hub_sums = jnp.sum(rows * (peaks * peaks), axis=0, keepdims=True)
            hub_mean = column(hub_sums, 2) / node_total
            authority[...] = authority_raw[...] * (
                first_scale / jnp.sqrt(authority_mean + EPS)
            )
            hub[...] = hub_raw[...] * (first_scale / jnp.sqrt(hub_mean + EPS))

        def shape(dims, kind):
            return jax.ShapeDtypeStruct(dims, kind)

        block_shape = (columns, edge)
        source_blocks = pltpu.VMEM((blocks + 1,) + block_shape, F32)
        source_slots = pltpu.VMEM((slot_total + 1,) + block_shape, F32)
        sum_blocks = pltpu.VMEM((blocks,) + block_shape, F32)
        sum_slots = pltpu.VMEM((slot_total,) + block_shape, F32)
        whole = shape((columns, blocks * edge), F32)
        plain = shape((devices, rows_each, edge), BF16)
        square_shape = shape(block_shape, F32)

        def exchange(value):
            return lax.all_to_all(value, "rows", split_axis=0, concat_axis=0, tiled=True)

        send, tiles = pl.pallas_call(
            start_kernel,
            name="start",
            out_shape=(
                shape((devices, rows_each + columns, edge), BF16),
                shape(edge_tiles.shape, edge_tiles.dtype),
            ),
            in_specs=[smem, smem, smem, smem, vmem, hbm],
            out_specs=(vmem, vmem),
            scratch_shapes=[source_blocks, sum_slots, pltpu.SemaphoreType.DMA((tile_total // chunk,))],
            compiler_params=params,
        )(
            tile_count, tile_row, tile_slot, fetch_list, hub_start,
            pltpu.with_memory_space_constraint(edge_tiles, pltpu.HBM),
        )
        first = exchange(send)

        def owner(got):
            return pl.pallas_call(
                owner_kernel,
                name="owner",
                out_shape=(whole, plain, square_shape),
                in_specs=[vmem, vmem],
                out_specs=(vmem, vmem, vmem),
                compiler_params=params,
            )(got, first)

        _, reply, _ = owner(first)
        send, first_squares = pl.pallas_call(
            middle_kernel,
            name="middle",
            out_shape=(plain, square_shape),
            in_specs=[smem, smem, smem, vmem, vmem],
            out_specs=(vmem, vmem),
            scratch_shapes=[source_slots, sum_blocks, sum_slots, source_blocks],
            compiler_params=params,
        )(tile_count, tile_row, tile_slot, exchange(reply), tiles)
        authority_raw, reply, authority_squares = owner(exchange(send))
        hub_raw, send = pl.pallas_call(
            last_kernel,
            name="last",
            out_shape=(whole, shape((devices, edge), F32)),
            in_specs=[smem, smem, smem, vmem, vmem, vmem, vmem],
            out_specs=(vmem, vmem),
            scratch_shapes=[source_slots, sum_blocks],
            compiler_params=params,
        )(tile_count, tile_row, tile_slot, exchange(reply), tiles, first_squares, authority_squares)
        return pl.pallas_call(
            finish_kernel,
            name="finish",
            out_shape=(whole, whole),
            in_specs=[vmem, vmem, vmem],
            out_specs=(vmem, vmem),
            compiler_params=params,
        )(exchange(send), hub_raw, authority_raw)

    in_specs = (
        P("rows", None, None),
        P("rows"),
        P("rows"),
        P("rows"),
        P("rows", None),
        P(None, "rows"),
    )
    out_specs = (P(None, "rows"), P(None, "rows"))
    return jax.shard_map(
        per_device, mesh=mesh, in_specs=in_specs, out_specs=out_specs, check_vma=False
    )
```

```python
import math

import jax
import jax.numpy as jnp
from jax import lax
from jax.experimental import pallas as pl
from jax.experimental.pallas import tpu as pltpu
from jax.sharding import PartitionSpec as P

ITERS = 2
EPS = 1e-06
GROUP = 8
COPY_TILES = 32
STEP_TILES = 64
VMEM_LIMIT = 24 * 1024 * 1024

F32 = jnp.float32
BF16 = jnp.bfloat16


def tile_sweep(transposed, count, row_s, slot_s, tiles, source, accum, chunk, group, arrive):
    zero_at = source.shape[0] - 1
    columns, edge = source.shape[1:]
    half = group // 2
    pick, put = (row_s, slot_s) if transposed else (slot_s, row_s)

    def one_group(base):
        blocks = []
        targets = []
        for t in range(group):
            at = base + t
            blocks.append(source[jnp.where(at < count, pick[at], zero_at)])
            targets.append(put[at])
        pad = jnp.zeros((columns * half, edge), F32)
        left = jnp.concatenate(
            [
                jnp.concatenate(blocks[0::2] + [pad], 0),
                jnp.concatenate([pad] + blocks[1::2], 0),
            ],
            1,
        ).astype(BF16)
        weights = [tiles[base + t] for t in range(group)]
        outer, inner = (1, 0) if transposed else (0, 1)
        right = jnp.concatenate(
            [jnp.concatenate(weights[0::2], outer), jnp.concatenate(weights[1::2], outer)], inner
        )
        product = lax.dot_general(
            left, right, (((1,), (inner,)), ((), ())), preferred_element_type=F32
        )
        for t in range(group):
            first = (t % 2) * columns * half + (t // 2) * columns
            lane = (t // 2) * edge
            accum[targets[t]] += product[first : first + columns, lane : lane + edge]

    def one_chunk(c, carry):
        arrive(c)

        for g in range(chunk // group):
            one_group(c * chunk + g * group)
        return carry

    lax.fori_loop(0, (count + chunk - 1) // chunk, one_chunk, 0)


def pack_blocks(accum, send, devices, slots_each):
    columns = accum.shape[1]
    for p in range(devices):
        both = jnp.concatenate([accum[p * slots_each + k] for k in range(slots_each)], 0)
        send[p, : slots_each * columns, :] = both.astype(BF16)


def solution(mesh):
    devices = mesh.shape["rows"]

    def per_device(edge_tiles, tile_row, tile_slot, tile_count, fetch_list, hub_start):
        tile_total, edge, _ = edge_tiles.shape
        columns = hub_start.shape[0]
        blocks = hub_start.shape[1] // edge
        slot_total = fetch_list.shape[1]
        slots_each = slot_total // devices
        node_total = hub_start.shape[1] * devices
        chunk = math.gcd(COPY_TILES, tile_total)
        step = math.gcd(STEP_TILES, tile_total)
        group = math.gcd(GROUP, chunk)
        always = min(2, tile_total // chunk)
        rows_each = slots_each * columns
        assert blocks**slots_each <= 256 and group % 2 == 0

        smem = pl.BlockSpec(memory_space=pltpu.SMEM)
        vmem = pl.BlockSpec(memory_space=pltpu.VMEM)
        hbm = pl.BlockSpec(memory_space=pltpu.HBM)
        params = pltpu.CompilerParams(vmem_limit_bytes=VMEM_LIMIT)

        def start_kernel(
            cnt, row_hbm, slot_hbm, fetch_hbm, hub_hbm, tiles,
            send, kept, row_s, slot_s, fetch, hub, source, accum, sems, small
        ):
            def copy(c):
                span = pl.ds(c * chunk, chunk)
                return pltpu.make_async_copy(tiles.at[span], kept.at[span], sems.at[c])

            def begin(c, carry):
                copy(c).start()
                return carry

            def end(c, carry):
                copy(c).wait()
                return carry

            pairs = [(hub_hbm, hub), (row_hbm, row_s), (slot_hbm, slot_s), (fetch_hbm, fetch)]
            parts = [pltpu.make_async_copy(a, b, small.at[i]) for i, (a, b) in enumerate(pairs)]
            for part in parts:
                part.start()
            for c in range(always):
                copy(c).start()
            accum[...] = jnp.zeros_like(accum)
            source[blocks] = jnp.zeros((columns, edge), F32)
            count = cnt[0]
            live = (count + chunk - 1) // chunk
            lax.fori_loop(always, live, begin, 0)
            for part in parts:
                part.wait()
            for b in range(blocks):
                source[b] = hub[:, b * edge : (b + 1) * edge].astype(BF16).astype(F32)
            tile_sweep(
                True, count, row_s, slot_s, kept, source, accum, chunk, group,
                lambda c: copy(c).wait(),
            )
            lax.fori_loop(live, always, end, 0)
            pack_blocks(accum, send, devices, slots_each)
            for p in range(devices):
                code = fetch[0, p * slots_each]
                for k in range(1, slots_each):
                    code = code + fetch[0, p * slots_each + k] * blocks**k
                send[p, rows_each:, :] = (
                    jnp.full((columns, edge), code, jnp.int32).astype(F32).astype(BF16)
                )

        def owner_kernel(got, codes, reply, raw=None, squares=None):
            totals = [jnp.zeros((columns, edge), F32) for _ in range(blocks)]

            def entries(p):
                code = codes[p, rows_each:, :].astype(F32)
                wanted = []
                for k in range(slots_each - 1, 0, -1):
                    high = jnp.floor(code * (1.0 / blocks**k))
                    wanted.append(high)
                    code = code - high * blocks**k
                return (wanted + [code])[::-1]

            for p in range(devices):
                wanted = entries(p)
                values = got[p, :rows_each, :].astype(F32)
                for k in range(slots_each):
                    value = values[k * columns : (k + 1) * columns]
                    for b in range(blocks):
                        totals[b] = totals[b] + jnp.where(wanted[k] == b, value, 0.0)
            if raw is not None:
                square = jnp.zeros((columns, edge), F32)
                for b in range(blocks):
                    raw[:, b * edge : (b + 1) * edge] = totals[b]
                    square = square + totals[b] * totals[b]
                squares[...] = square
            for p in range(devices):
                wanted = entries(p)
                out = []
                for k in range(slots_each):
                    chosen = totals[0]
                    for b in range(1, blocks):
                        chosen = jnp.where(wanted[k] == b, totals[b], chosen)
                    out.append(chosen)
                reply[p] = jnp.concatenate(out, 0).astype(BF16)

        def load_fetched(fetched, source):
            for p in range(devices):
                both = fetched[p].astype(F32)
                for k in range(slots_each):
                    source[p * slots_each + k] = both[k * columns : (k + 1) * columns]
            source[slot_total] = jnp.zeros((columns, edge), F32)

        def middle_kernel(cnt, row_s, slot_s, fetched, tiles, send, squares, source, hub, accum, low):
            count = cnt[0]
            load_fetched(fetched, source)
            hub[...] = jnp.zeros_like(hub)
            accum[...] = jnp.zeros_like(accum)
            tile_sweep(
                False, count, row_s, slot_s, tiles, source, hub, step, group, lambda c: None
            )
            square = jnp.zeros((columns, edge), F32)
            for b in range(blocks):
                value = hub[b]
                square = square + value * value
                low[b] = value.astype(BF16).astype(F32)
            low[blocks] = jnp.zeros((columns, edge), F32)
            squares[...] = square
            tile_sweep(
                True, count, row_s, slot_s, tiles, low, accum, step, group, lambda c: None
            )
            pack_blocks(accum, send, devices, slots_each)

        def last_kernel(cnt, row_s, slot_s, fetched, tiles, first_squares, authority_squares, raw, send, source, hub):
            count = cnt[0]
            load_fetched(fetched, source)
            hub[...] = jnp.zeros_like(hub)
            tile_sweep(
                False, count, row_s, slot_s, tiles, source, hub, step, group, lambda c: None
            )
            largest = jnp.zeros((columns, edge), F32)
            for b in range(blocks):
                largest = jnp.maximum(largest, jnp.abs(hub[b]))
            peak = jnp.max(largest, axis=1, keepdims=True)
            inverse = jnp.where(peak > 1e-30, 1.0 / jnp.maximum(peak, 1e-30), 0.0)
            square = jnp.zeros((columns, edge), F32)
            for b in range(blocks):
                value = hub[b]
                raw[:, b * edge : (b + 1) * edge] = value
                scaled = value * inverse
                square = square + scaled * scaled
            stats = [
                jnp.sum(first_squares[...], axis=1, keepdims=True),
                jnp.sum(authority_squares[...], axis=1, keepdims=True),
                jnp.sum(square, axis=1, keepdims=True),
                peak,
            ]
            lane = lax.broadcasted_iota(jnp.int32, (columns, edge), 1)
            sub = lax.broadcasted_iota(jnp.int32, (columns, edge), 0)
            mixed = jnp.zeros((columns, edge), F32)
            for j, stat in enumerate(stats):
                mixed = jnp.where(lane == sub + j * columns, stat, mixed)
            line = jnp.sum(mixed, axis=0, keepdims=True)
            send[...] = jnp.broadcast_to(line, send.shape)

        def finish_kernel(got, hub_raw, authority_raw, hub, authority):
            rows = got[...]
            lane = lax.broadcasted_iota(jnp.int32, (columns, edge), 1)
            sub = lax.broadcasted_iota(jnp.int32, (columns, edge), 0)

            def column(line, j):
                spread = jnp.broadcast_to(line, (columns, edge))
                kept = jnp.where(lane == sub + j * columns, spread, 0.0)
                return jnp.sum(kept, axis=1, keepdims=True)

            sums = jnp.sum(rows, axis=0, keepdims=True)
            first = column(sums, 0) / node_total
            first_scale = 1.0 / jnp.sqrt(first + EPS)
            authority_mean = column(sums, 1) / node_total * first_scale * first_scale
            at_peaks = jnp.sum(
                jnp.where(lane == sub + 3 * columns, first_scale, 0.0), axis=0, keepdims=True
            )
            peaks = rows * at_peaks
            peaks = pltpu.roll(peaks, edge - columns, 1)
            hub_sums = jnp.sum(rows * (peaks * peaks), axis=0, keepdims=True)
            hub_mean = column(hub_sums, 2) / node_total
            authority[...] = authority_raw[...] * (
                first_scale / jnp.sqrt(authority_mean + EPS)
            )
            hub[...] = hub_raw[...] * (first_scale / jnp.sqrt(hub_mean + EPS))

        def shape(dims, kind):
            return jax.ShapeDtypeStruct(dims, kind)

        block_shape = (columns, edge)
        source_blocks = pltpu.VMEM((blocks + 1,) + block_shape, F32)
        source_slots = pltpu.VMEM((slot_total + 1,) + block_shape, F32)
        sum_blocks = pltpu.VMEM((blocks,) + block_shape, F32)
        sum_slots = pltpu.VMEM((slot_total,) + block_shape, F32)
        whole = shape((columns, blocks * edge), F32)
        plain = shape((devices, rows_each, edge), BF16)
        square_shape = shape(block_shape, F32)

        def exchange(value):
            return lax.all_to_all(value, "rows", split_axis=0, concat_axis=0, tiled=True)

        small = [tile_count, tile_row, tile_slot]
        operands = small + [fetch_list, hub_start, edge_tiles]
        send, tiles = pl.pallas_call(
            start_kernel,
            name="start",
            out_shape=(
                shape((devices, rows_each + columns, edge), BF16),
                shape(edge_tiles.shape, edge_tiles.dtype),
            ),
            in_specs=[smem] + [hbm] * 5,
            out_specs=(vmem, vmem),
            scratch_shapes=[
                *[pltpu.SMEM(a.shape, a.dtype) for a in small[1:]],
                pltpu.SMEM(fetch_list.shape, fetch_list.dtype),
                pltpu.VMEM(hub_start.shape, F32),
                source_blocks,
                sum_slots,
                pltpu.SemaphoreType.DMA((tile_total // chunk,)),
                pltpu.SemaphoreType.DMA((4,)),
            ],
            compiler_params=params,
        )(tile_count, *[pltpu.with_memory_space_constraint(a, pltpu.HBM) for a in operands[1:]])
        first = exchange(send)

        def owner(got, outputs):
            return pl.pallas_call(
                owner_kernel,
                name="owner",
                out_shape=(plain, whole, square_shape)[:outputs],
                in_specs=[vmem, vmem],
                out_specs=(vmem, vmem, vmem)[:outputs],
                compiler_params=params,
            )(got, first)

        (reply,) = owner(first, 1)
        send, first_squares = pl.pallas_call(
            middle_kernel,
            name="middle",
            out_shape=(plain, square_shape),
            in_specs=[smem, smem, smem, vmem, vmem],
            out_specs=(vmem, vmem),
            scratch_shapes=[source_slots, sum_blocks, sum_slots, source_blocks],
            compiler_params=params,
        )(*small, exchange(reply), tiles)
        reply, authority_raw, authority_squares = owner(exchange(send), 3)
        hub_raw, send = pl.pallas_call(
            last_kernel,
            name="last",
            out_shape=(whole, shape((devices, edge), F32)),
            in_specs=[smem, smem, smem, vmem, vmem, vmem, vmem],
            out_specs=(vmem, vmem),
            scratch_shapes=[source_slots, sum_blocks],
            compiler_params=params,
        )(*small, exchange(reply), tiles, first_squares, authority_squares)
        return pl.pallas_call(
            finish_kernel,
            name="finish",
            out_shape=(whole, whole),
            in_specs=[vmem, vmem, vmem],
            out_specs=(vmem, vmem),
            compiler_params=params,
        )(exchange(send), hub_raw, authority_raw)

    in_specs = (
        P("rows", None, None),
        P("rows"),
        P("rows"),
        P("rows"),
        P("rows", None),
        P(None, "rows"),
    )
    out_specs = (P(None, "rows"), P(None, "rows"))
    return jax.shard_map(
        per_device, mesh=mesh, in_specs=in_specs, out_specs=out_specs, check_vma=False
    )
```

```python
import functools
import math

import jax
import jax.numpy as jnp
from jax import lax
from jax.experimental import pallas as pl
from jax.experimental.pallas import tpu as pltpu
from jax.sharding import PartitionSpec as P

ITERS = 2
EPS = 1e-06
GROUP = 8
COPY_TILES = 32
STEP_TILES = 64
VMEM_LIMIT = 28 * 1024 * 1024

F32 = jnp.float32
BF16 = jnp.bfloat16


def tile_sweep(
    rounds, chunk, group, count, pick, put, tiles, source, accum, before=None, beside=None
):
    zero_at = source.shape[0] - 1
    columns, edge = source.shape[1:]
    half = group // 2

    def one_group(base):
        blocks = []
        targets = []
        for t in range(group):
            at = base + t
            blocks.append(source[jnp.where(at < count, pick[at], zero_at)])
            targets.append(put[at])
        pad = jnp.zeros((columns * half, edge), F32)
        left = jnp.concatenate(
            [
                jnp.concatenate(blocks[0::2] + [pad], 0),
                jnp.concatenate([pad] + blocks[1::2], 0),
            ],
            1,
        ).astype(BF16)
        weights = [tiles[base + t] for t in range(group)]
        right = jnp.concatenate(
            [jnp.concatenate(weights[0::2], 1), jnp.concatenate(weights[1::2], 1)], 0
        )
        product = jnp.dot(left, right, preferred_element_type=F32)
        for t in range(group):
            first = (t % 2) * columns * half + (t // 2) * columns
            lane = (t // 2) * edge
            accum[targets[t]] += product[first : first + columns, lane : lane + edge]

    def one_chunk(c, carry):
        if before is not None:
            before(c)
        for g in range(chunk // group):
            one_group(c * chunk + g * group)
            if beside is not None:
                for t in range(group):
                    beside(c * chunk + g * group + t)
        return carry

    lax.fori_loop(0, rounds, one_chunk, 0)


def pack_blocks(accum, send, devices, slots_each):
    columns = accum.shape[1]
    for p in range(devices):
        both = jnp.concatenate([accum[p * slots_each + k] for k in range(slots_each)], 0)
        send[p, : slots_each * columns, :] = both.astype(BF16)


def solution(mesh):
    devices = mesh.shape["rows"]

    def per_device(edge_tiles, tile_row, tile_slot, tile_count, fetch_list, hub_start):
        tile_total, edge, _ = edge_tiles.shape
        columns = hub_start.shape[0]
        blocks = hub_start.shape[1] // edge
        slot_total = fetch_list.shape[1]
        slots_each = slot_total // devices
        node_total = hub_start.shape[1] * devices
        step = math.gcd(STEP_TILES, tile_total)
        chunk = math.gcd(COPY_TILES, step)
        group = math.gcd(GROUP, chunk)
        always = min(2, tile_total // chunk)
        rows_each = slots_each * columns
        rows_first = rows_each + slots_each + slots_each % 2
        assert group % 2 == 0

        smem = pl.BlockSpec(memory_space=pltpu.SMEM)
        vmem = pl.BlockSpec(memory_space=pltpu.VMEM)
        hbm = pl.BlockSpec(memory_space=pltpu.HBM)
        params = pltpu.CompilerParams(vmem_limit_bytes=VMEM_LIMIT)

        def start_kernel(
            cnt, row_hbm, slot_hbm, fetch_hbm, hub_hbm, tiles,
            send, kept, flipped, live_count, row_s, slot_s, fetch, hub, source, accum, sems, small
        ):
            def copy(c):
                span = pl.ds(c * chunk, chunk)
                return pltpu.make_async_copy(tiles.at[span], kept.at[span], sems.at[c])

            def begin(c, carry):
                copy(c).start()
                return carry

            def end(c, carry):
                copy(c).wait()
                return carry

            pairs = [(hub_hbm, hub), (row_hbm, row_s), (slot_hbm, slot_s), (fetch_hbm, fetch)]
            parts = [pltpu.make_async_copy(a, b, small.at[i]) for i, (a, b) in enumerate(pairs)]
            for part in parts:
                part.start()
            for c in range(always):
                copy(c).start()
            accum[...] = jnp.zeros_like(accum)
            source[blocks] = jnp.zeros((columns, edge), F32)
            count = cnt[0]
            live_count[...] = jnp.full(live_count.shape, count, jnp.int32)
            live = (count + step - 1) // step * (step // chunk)
            lax.fori_loop(always, live, begin, 0)
            for part in parts:
                part.wait()

            def flip(i):
                flipped[i] = kept[i].T

            for b in range(blocks):
                source[b] = hub[:, b * edge : (b + 1) * edge].astype(BF16).astype(F32)
            tile_sweep(
                live, chunk, group, count, row_s, slot_s, kept, source, accum,
                lambda c: copy(c).wait(), flip,
            )
            lax.fori_loop(live, always, end, 0)
            for p in range(devices):
                base = p * rows_first
                both = [accum[p * slots_each + k] for k in range(slots_each)]
                send[base : base + rows_each] = jnp.concatenate(both, 0).astype(BF16)
                wanted = [
                    jnp.full((1, edge), fetch[0, p * slots_each + k % slots_each], jnp.int32)
                    for k in range(rows_first - rows_each)
                ]
                send[base + rows_each : base + rows_first] = (
                    jnp.concatenate(wanted, 0).astype(F32).astype(BF16)
                )

        def owner_kernel(got_rows, got, first, reply, raw=None, squares=None):
            totals = [jnp.zeros((columns, edge), F32) for _ in range(blocks)]

            def wanted_blocks(p):
                base = p * rows_first
                rows = first[base + rows_each : base + rows_first].astype(F32)
                return [
                    jnp.broadcast_to(rows[k : k + 1], (columns, edge)) for k in range(slots_each)
                ]

            for p in range(devices):
                wanted = wanted_blocks(p)
                values = got[p * got_rows : p * got_rows + rows_each].astype(F32)
                for k in range(slots_each):
                    value = values[k * columns : (k + 1) * columns]
                    for b in range(blocks):
                        totals[b] = totals[b] + jnp.where(wanted[k] == b, value, 0.0)
            if raw is not None:
                square = jnp.zeros((columns, edge), F32)
                for b in range(blocks):
                    raw[:, b * edge : (b + 1) * edge] = totals[b]
                    square = square + totals[b] * totals[b]
                squares[...] = square
            for p in range(devices):
                wanted = wanted_blocks(p)
                out = []
                for k in range(slots_each):
                    chosen = totals[0]
                    for b in range(1, blocks):
                        chosen = jnp.where(wanted[k] == b, totals[b], chosen)
                    out.append(chosen)
                reply[p] = jnp.concatenate(out, 0).astype(BF16)

        def load_fetched(fetched, source):
            for p in range(devices):
                both = fetched[p].astype(F32)
                for k in range(slots_each):
                    source[p * slots_each + k] = both[k * columns : (k + 1) * columns]
            source[slot_total] = jnp.zeros((columns, edge), F32)

        def middle_kernel(
            cnt, row_s, slot_s, fetched, tiles, flipped,
            send, squares, source, hub, accum, low
        ):
            count = cnt[0, 0]
            rounds = (count + step - 1) // step
            load_fetched(fetched, source)
            hub[...] = jnp.zeros_like(hub)
            accum[...] = jnp.zeros_like(accum)
            tile_sweep(rounds, step, group, count, slot_s, row_s, flipped, source, hub)
            square = jnp.zeros((columns, edge), F32)
            for b in range(blocks):
                value = hub[b]
                square = square + value * value
                low[b] = value.astype(BF16).astype(F32)
            low[blocks] = jnp.zeros((columns, edge), F32)
            squares[...] = square
            tile_sweep(rounds, step, group, count, row_s, slot_s, tiles, low, accum)
            pack_blocks(accum, send, devices, slots_each)

        def last_kernel(
            cnt, row_s, slot_s, fetched, flipped, first_squares, authority_squares,
            raw, send, source, hub
        ):
            count = cnt[0, 0]
            rounds = (count + step - 1) // step
            load_fetched(fetched, source)
            hub[...] = jnp.zeros_like(hub)
            tile_sweep(rounds, step, group, count, slot_s, row_s, flipped, source, hub)
            largest = jnp.zeros((columns, edge), F32)
            for b in range(blocks):
                largest = jnp.maximum(largest, jnp.abs(hub[b]))
            peak = jnp.max(largest, axis=1, keepdims=True)
            inverse = jnp.where(peak > 1e-30, 1.0 / jnp.maximum(peak, 1e-30), 0.0)
            square = jnp.zeros((columns, edge), F32)
            for b in range(blocks):
                value = hub[b]
                raw[:, b * edge : (b + 1) * edge] = value
                scaled = value * inverse
                square = square + scaled * scaled
            stats = [
                jnp.sum(first_squares[...], axis=1, keepdims=True),
                jnp.sum(authority_squares[...], axis=1, keepdims=True),
                jnp.sum(square, axis=1, keepdims=True),
                peak,
            ]
            lane = lax.broadcasted_iota(jnp.int32, (columns, edge), 1)
            sub = lax.broadcasted_iota(jnp.int32, (columns, edge), 0)
            mixed = jnp.zeros((columns, edge), F32)
            for j, stat in enumerate(stats):
                mixed = jnp.where(lane == sub + j * columns, stat, mixed)
            line = jnp.sum(mixed, axis=0, keepdims=True)
            send[...] = jnp.broadcast_to(line, send.shape)

        def finish_kernel(got, hub_raw, authority_raw, hub, authority):
            rows = got[...]
            lane = lax.broadcasted_iota(jnp.int32, (columns, edge), 1)
            sub = lax.broadcasted_iota(jnp.int32, (columns, edge), 0)

            def column(line, j):
                spread = jnp.broadcast_to(line, (columns, edge))
                kept = jnp.where(lane == sub + j * columns, spread, 0.0)
                return jnp.sum(kept, axis=1, keepdims=True)

            sums = jnp.sum(rows, axis=0, keepdims=True)
            first = column(sums, 0) / node_total
            first_scale = 1.0 / jnp.sqrt(first + EPS)
            authority_mean = column(sums, 1) / node_total * first_scale * first_scale
            at_peaks = jnp.sum(
                jnp.where(lane == sub + 3 * columns, first_scale, 0.0), axis=0, keepdims=True
            )
            peaks = rows * at_peaks
            peaks = pltpu.roll(peaks, edge - columns, 1)
            hub_sums = jnp.sum(rows * (peaks * peaks), axis=0, keepdims=True)
            hub_mean = column(hub_sums, 2) / node_total
            authority[...] = authority_raw[...] * (
                first_scale / jnp.sqrt(authority_mean + EPS)
            )
            hub[...] = hub_raw[...] * (first_scale / jnp.sqrt(hub_mean + EPS))

        def shape(dims, kind):
            return jax.ShapeDtypeStruct(dims, kind)

        block_shape = (columns, edge)
        source_blocks = pltpu.VMEM((blocks + 1,) + block_shape, F32)
        source_slots = pltpu.VMEM((slot_total + 1,) + block_shape, F32)
        sum_blocks = pltpu.VMEM((blocks,) + block_shape, F32)
        sum_slots = pltpu.VMEM((slot_total,) + block_shape, F32)
        whole = shape((columns, blocks * edge), F32)
        plain = shape((devices, rows_each, edge), BF16)
        square_shape = shape(block_shape, F32)

        def exchange(value):
            return lax.all_to_all(value, "rows", split_axis=0, concat_axis=0, tiled=True)

        small = [tile_count, tile_row, tile_slot]
        operands = small + [fetch_list, hub_start, edge_tiles]
        send, tiles, flipped, live_count = pl.pallas_call(
            start_kernel,
            name="start",
            out_shape=(
                shape((devices * rows_first, edge), BF16),
                shape(edge_tiles.shape, edge_tiles.dtype),
                shape(edge_tiles.shape, edge_tiles.dtype),
                shape((1, edge), jnp.int32),
            ),
            in_specs=[smem] + [hbm] * 5,
            out_specs=(vmem,) * 4,
            scratch_shapes=[
                *[pltpu.SMEM(a.shape, a.dtype) for a in small[1:]],
                pltpu.SMEM(fetch_list.shape, fetch_list.dtype),
                pltpu.VMEM(hub_start.shape, F32),
                source_blocks,
                sum_slots,
                pltpu.SemaphoreType.DMA((tile_total // chunk,)),
                pltpu.SemaphoreType.DMA((4,)),
            ],
            compiler_params=params,
        )(tile_count, *[pltpu.with_memory_space_constraint(a, pltpu.HBM) for a in operands[1:]])
        halves = (devices, rows_first // 2, 2, edge)
        first = exchange(send.reshape(halves)).reshape(send.shape)
        small = [live_count, tile_row, tile_slot]

        def owner(got, outputs):
            return pl.pallas_call(
                functools.partial(owner_kernel, got.shape[0] // devices),
                name="owner",
                out_shape=(plain, whole, square_shape)[:outputs],
                in_specs=[vmem, vmem],
                out_specs=(vmem, vmem, vmem)[:outputs],
                compiler_params=params,
            )(got, first)

        (reply,) = owner(first, 1)
        send, first_squares = pl.pallas_call(
            middle_kernel,
            name="middle",
            out_shape=(plain, square_shape),
            in_specs=[smem, smem, smem, vmem, vmem, vmem],
            out_specs=(vmem, vmem),
            scratch_shapes=[source_slots, sum_blocks, sum_slots, source_blocks],
            compiler_params=params,
        )(*small, exchange(reply), tiles, flipped)
        reply, authority_raw, authority_squares = owner(exchange(send).reshape(devices * rows_each, edge), 3)
        hub_raw, send = pl.pallas_call(
            last_kernel,
            name="last",
            out_shape=(whole, shape((devices, edge), F32)),
            in_specs=[smem, smem, smem, vmem, vmem, vmem, vmem],
            out_specs=(vmem, vmem),
            scratch_shapes=[source_slots, sum_blocks],
            compiler_params=params,
        )(*small, exchange(reply), flipped, first_squares, authority_squares)
        return pl.pallas_call(
            finish_kernel,
            name="finish",
            out_shape=(whole, whole),
            in_specs=[vmem, vmem, vmem],
            out_specs=(vmem, vmem),
            compiler_params=params,
        )(exchange(send), hub_raw, authority_raw)

    in_specs = (
        P("rows", None, None),
        P("rows"),
        P("rows"),
        P("rows"),
        P("rows", None),
        P(None, "rows"),
    )
    out_specs = (P(None, "rows"), P(None, "rows"))
    return jax.shard_map(
        per_device, mesh=mesh, in_specs=in_specs, out_specs=out_specs, check_vma=False
    )
```

```python
import functools
import math

import jax
import jax.numpy as jnp
from jax import lax
from jax.experimental import pallas as pl
from jax.experimental.pallas import tpu as pltpu
from jax.sharding import PartitionSpec as P

ITERS = 2
EPS = 1e-06
GROUP = 2
COPY_TILES = 32
STEP_TILES = 64
VMEM_LIMIT = 28 * 1024 * 1024

F32 = jnp.float32
BF16 = jnp.bfloat16


def tile_sweep(
    live, chunk, group, count, pick, put, tiles, source, accum, before=None, beside=None
):
    zero_at = source.shape[0] - 1
    columns, edge = source.shape[1:]
    half = group // 2

    def one_group(base):
        blocks = []
        targets = []
        for t in range(group):
            at = base + t
            blocks.append(source[jnp.where(at < count, pick[at], zero_at)])
            targets.append(put[at])
        pad = jnp.zeros((columns * half, edge), F32)
        left = jnp.concatenate(
            [
                jnp.concatenate(blocks[0::2] + [pad], 0),
                jnp.concatenate([pad] + blocks[1::2], 0),
            ],
            1,
        ).astype(BF16)
        weights = [tiles[base + t] for t in range(group)]
        right = jnp.concatenate(
            [jnp.concatenate(weights[0::2], 1), jnp.concatenate(weights[1::2], 1)], 0
        )
        product = jnp.dot(left, right, preferred_element_type=F32)
        for t in range(group):
            first = (t % 2) * columns * half + (t // 2) * columns
            lane = (t // 2) * edge
            accum[targets[t]] += product[first : first + columns, lane : lane + edge]

    def one_chunk(c, carry):
        if before is not None:
            before(c)
        for g in range(chunk // group):
            one_group(c * chunk + g * group)
            if beside is not None:
                for t in range(group):
                    beside(c * chunk + g * group + t)
        return carry

    chunks = tiles.shape[0] // chunk

    if before is not None:
        lax.fori_loop(0, live, one_chunk, 0)
        return

    @pl.when(live == chunks)
    def _():
        for c in range(chunks):
            one_chunk(c, 0)

    @pl.when(live < chunks)
    def _():
        lax.fori_loop(0, live, one_chunk, 0)


def pack_blocks(accum, send, devices, slots_each):
    columns = accum.shape[1]
    for p in range(devices):
        both = jnp.concatenate([accum[p * slots_each + k] for k in range(slots_each)], 0)
        send[p, : slots_each * columns, :] = both.astype(BF16)


def solution(mesh):
    devices = mesh.shape["rows"]

    def per_device(edge_tiles, tile_row, tile_slot, tile_count, fetch_list, hub_start):
        tile_total, edge, _ = edge_tiles.shape
        columns = hub_start.shape[0]
        blocks = hub_start.shape[1] // edge
        slot_total = fetch_list.shape[1]
        slots_each = slot_total // devices
        node_total = hub_start.shape[1] * devices
        step = math.gcd(STEP_TILES, tile_total)
        chunk = math.gcd(COPY_TILES, step)
        group = math.gcd(GROUP, chunk)
        always = min(2, tile_total // chunk)
        rows_each = slots_each * columns
        rows_first = rows_each + slots_each + slots_each % 2
        assert group % 2 == 0

        smem = pl.BlockSpec(memory_space=pltpu.SMEM)
        vmem = pl.BlockSpec(memory_space=pltpu.VMEM)
        hbm = pl.BlockSpec(memory_space=pltpu.HBM)
        params = pltpu.CompilerParams(vmem_limit_bytes=VMEM_LIMIT)

        def start_kernel(
            cnt, row_hbm, slot_hbm, fetch_hbm, hub_hbm, tiles,
            send, kept, flipped, live_count, row_s, slot_s, fetch, hub, source, accum, sems, small
        ):
            def copy(c):
                span = pl.ds(c * chunk, chunk)
                return pltpu.make_async_copy(tiles.at[span], kept.at[span], sems.at[c])

            def begin(c, carry):
                copy(c).start()
                return carry

            def end(c, carry):
                copy(c).wait()
                return carry

            pairs = [(hub_hbm, hub), (row_hbm, row_s), (slot_hbm, slot_s), (fetch_hbm, fetch)]
            parts = [pltpu.make_async_copy(a, b, small.at[i]) for i, (a, b) in enumerate(pairs)]
            for part in parts:
                part.start()
            for c in range(always):
                copy(c).start()
            accum[...] = jnp.zeros_like(accum)
            source[blocks] = jnp.zeros((columns, edge), F32)
            count = cnt[0]
            live_count[...] = jnp.full(live_count.shape, count, jnp.int32)
            live = (count + step - 1) // step * (step // chunk)
            lax.fori_loop(always, live, begin, 0)
            for part in parts:
                part.wait()

            def flip(i):
                flipped[i] = kept[i].T

            for b in range(blocks):
                source[b] = hub[:, b * edge : (b + 1) * edge].astype(BF16).astype(F32)
            tile_sweep(
                live, chunk, group, count, row_s, slot_s, kept, source, accum,
                lambda c: copy(c).wait(), flip,
            )
            lax.fori_loop(live, always, end, 0)
            for p in range(devices):
                base = p * rows_first
                both = [accum[p * slots_each + k] for k in range(slots_each)]
                send[base : base + rows_each] = jnp.concatenate(both, 0).astype(BF16)
                wanted = [
                    jnp.full((1, edge), fetch[0, p * slots_each + k % slots_each], jnp.int32)
                    for k in range(rows_first - rows_each)
                ]
                send[base + rows_each : base + rows_first] = (
                    jnp.concatenate(wanted, 0).astype(F32).astype(BF16)
                )

        def owner_kernel(got_rows, got, first, reply, raw=None, squares=None):
            totals = [jnp.zeros((columns, edge), F32) for _ in range(blocks)]

            def wanted_blocks(p):
                base = p * rows_first
                rows = first[base + rows_each : base + rows_first].astype(F32)
                return [
                    jnp.broadcast_to(rows[k : k + 1], (columns, edge)) for k in range(slots_each)
                ]

            for p in range(devices):
                wanted = wanted_blocks(p)
                values = got[p * got_rows : p * got_rows + rows_each].astype(F32)
                for k in range(slots_each):
                    value = values[k * columns : (k + 1) * columns]
                    for b in range(blocks):
                        totals[b] = totals[b] + jnp.where(wanted[k] == b, value, 0.0)
            if raw is not None:
                square = jnp.zeros((columns, edge), F32)
                for b in range(blocks):
                    raw[:, b * edge : (b + 1) * edge] = totals[b]
                    square = square + totals[b] * totals[b]
                squares[...] = square
            for p in range(devices):
                wanted = wanted_blocks(p)
                out = []
                for k in range(slots_each):
                    chosen = totals[0]
                    for b in range(1, blocks):
                        chosen = jnp.where(wanted[k] == b, totals[b], chosen)
                    out.append(chosen)
                reply[p] = jnp.concatenate(out, 0).astype(BF16)

        def load_fetched(fetched, source):
            for p in range(devices):
                both = fetched[p].astype(F32)
                for k in range(slots_each):
                    source[p * slots_each + k] = both[k * columns : (k + 1) * columns]
            source[slot_total] = jnp.zeros((columns, edge), F32)

        def middle_kernel(
            cnt, row_s, slot_s, fetched, tiles, flipped,
            send, squares, source, hub, accum, low
        ):
            count = cnt[0, 0]
            rounds = (count + step - 1) // step
            load_fetched(fetched, source)
            hub[...] = jnp.zeros_like(hub)
            accum[...] = jnp.zeros_like(accum)
            tile_sweep(rounds, step, group, count, slot_s, row_s, flipped, source, hub)
            square = jnp.zeros((columns, edge), F32)
            for b in range(blocks):
                value = hub[b]
                square = square + value * value
                low[b] = value.astype(BF16).astype(F32)
            low[blocks] = jnp.zeros((columns, edge), F32)
            squares[...] = square
            tile_sweep(rounds, step, group, count, row_s, slot_s, tiles, low, accum)
            pack_blocks(accum, send, devices, slots_each)

        def last_kernel(
            cnt, row_s, slot_s, fetched, flipped, first_squares, authority_squares,
            raw, send, source, hub
        ):
            count = cnt[0, 0]
            rounds = (count + step - 1) // step
            load_fetched(fetched, source)
            hub[...] = jnp.zeros_like(hub)
            tile_sweep(rounds, step, group, count, slot_s, row_s, flipped, source, hub)
            largest = jnp.zeros((columns, edge), F32)
            for b in range(blocks):
                largest = jnp.maximum(largest, jnp.abs(hub[b]))
            peak = jnp.max(largest, axis=1, keepdims=True)
            inverse = jnp.where(peak > 1e-30, 1.0 / jnp.maximum(peak, 1e-30), 0.0)
            square = jnp.zeros((columns, edge), F32)
            for b in range(blocks):
                value = hub[b]
                raw[:, b * edge : (b + 1) * edge] = value
                scaled = value * inverse
                square = square + scaled * scaled
            stats = [
                jnp.sum(first_squares[...], axis=1, keepdims=True),
                jnp.sum(authority_squares[...], axis=1, keepdims=True),
                jnp.sum(square, axis=1, keepdims=True),
                peak,
            ]
            lane = lax.broadcasted_iota(jnp.int32, (columns, edge), 1)
            sub = lax.broadcasted_iota(jnp.int32, (columns, edge), 0)
            mixed = jnp.zeros((columns, edge), F32)
            for j, stat in enumerate(stats):
                mixed = jnp.where(lane == sub + j * columns, stat, mixed)
            line = jnp.sum(mixed, axis=0, keepdims=True)
            send[...] = jnp.broadcast_to(line, send.shape)

        def finish_kernel(got, hub_raw, authority_raw, hub, authority):
            rows = got[...]
            lane = lax.broadcasted_iota(jnp.int32, (columns, edge), 1)
            sub = lax.broadcasted_iota(jnp.int32, (columns, edge), 0)

            def column(line, j):
                spread = jnp.broadcast_to(line, (columns, edge))
                kept = jnp.where(lane == sub + j * columns, spread, 0.0)
                return jnp.sum(kept, axis=1, keepdims=True)

            sums = jnp.sum(rows, axis=0, keepdims=True)
            first = column(sums, 0) / node_total
            first_scale = 1.0 / jnp.sqrt(first + EPS)
            authority_mean = column(sums, 1) / node_total * first_scale * first_scale
            at_peaks = jnp.sum(
                jnp.where(lane == sub + 3 * columns, first_scale, 0.0), axis=0, keepdims=True
            )
            peaks = rows * at_peaks
            peaks = pltpu.roll(peaks, edge - columns, 1)
            hub_sums = jnp.sum(rows * (peaks * peaks), axis=0, keepdims=True)
            hub_mean = column(hub_sums, 2) / node_total
            authority[...] = authority_raw[...] * (
                first_scale / jnp.sqrt(authority_mean + EPS)
            )
            hub[...] = hub_raw[...] * (first_scale / jnp.sqrt(hub_mean + EPS))

        def shape(dims, kind):
            return jax.ShapeDtypeStruct(dims, kind)

        block_shape = (columns, edge)
        source_blocks = pltpu.VMEM((blocks + 1,) + block_shape, F32)
        source_slots = pltpu.VMEM((slot_total + 1,) + block_shape, F32)
        sum_blocks = pltpu.VMEM((blocks,) + block_shape, F32)
        sum_slots = pltpu.VMEM((slot_total,) + block_shape, F32)
        whole = shape((columns, blocks * edge), F32)
        plain = shape((devices, rows_each, edge), BF16)
        square_shape = shape(block_shape, F32)

        def exchange(value):
            return lax.all_to_all(value, "rows", split_axis=0, concat_axis=0, tiled=True)

        small = [tile_count, tile_row, tile_slot]
        operands = small + [fetch_list, hub_start, edge_tiles]
        send, tiles, flipped, live_count = pl.pallas_call(
            start_kernel,
            name="start",
            out_shape=(
                shape((devices * rows_first, edge), BF16),
                shape(edge_tiles.shape, edge_tiles.dtype),
                shape(edge_tiles.shape, edge_tiles.dtype),
                shape((1, edge), jnp.int32),
            ),
            in_specs=[smem] + [hbm] * 5,
            out_specs=(vmem,) * 4,
            scratch_shapes=[
                *[pltpu.SMEM(a.shape, a.dtype) for a in small[1:]],
                pltpu.SMEM(fetch_list.shape, fetch_list.dtype),
                pltpu.VMEM(hub_start.shape, F32),
                source_blocks,
                sum_slots,
                pltpu.SemaphoreType.DMA((tile_total // chunk,)),
                pltpu.SemaphoreType.DMA((4,)),
            ],
            compiler_params=params,
        )(tile_count, *[pltpu.with_memory_space_constraint(a, pltpu.HBM) for a in operands[1:]])
        halves = (devices, rows_first // 2, 2, edge)
        first = exchange(send.reshape(halves)).reshape(send.shape)
        small = [live_count, tile_row, tile_slot]

        def owner(got, outputs):
            return pl.pallas_call(
                functools.partial(owner_kernel, got.shape[0] // devices),
                name="owner",
                out_shape=(plain, whole, square_shape)[:outputs],
                in_specs=[vmem, vmem],
                out_specs=(vmem, vmem, vmem)[:outputs],
                compiler_params=params,
            )(got, first)

        (reply,) = owner(first, 1)
        send, first_squares = pl.pallas_call(
            middle_kernel,
            name="middle",
            out_shape=(plain, square_shape),
            in_specs=[smem, smem, smem, vmem, vmem, vmem],
            out_specs=(vmem, vmem),
            scratch_shapes=[source_slots, sum_blocks, sum_slots, source_blocks],
            compiler_params=params,
        )(*small, exchange(reply), tiles, flipped)
        reply, authority_raw, authority_squares = owner(exchange(send).reshape(devices * rows_each, edge), 3)
        hub_raw, send = pl.pallas_call(
            last_kernel,
            name="last",
            out_shape=(whole, shape((devices, edge), F32)),
            in_specs=[smem, smem, smem, vmem, vmem, vmem, vmem],
            out_specs=(vmem, vmem),
            scratch_shapes=[source_slots, sum_blocks],
            compiler_params=params,
        )(*small, exchange(reply), flipped, first_squares, authority_squares)
        return pl.pallas_call(
            finish_kernel,
            name="finish",
            out_shape=(whole, whole),
            in_specs=[vmem, vmem, vmem],
            out_specs=(vmem, vmem),
            compiler_params=params,
        )(exchange(send), hub_raw, authority_raw)

    in_specs = (
        P("rows", None, None),
        P("rows"),
        P("rows"),
        P("rows"),
        P("rows", None),
        P(None, "rows"),
    )
    out_specs = (P(None, "rows"), P(None, "rows"))
    return jax.shard_map(
        per_device, mesh=mesh, in_specs=in_specs, out_specs=out_specs, check_vma=False
    )
```

```python
import math

import jax
import jax.numpy as jnp
from jax import lax
from jax.experimental import pallas as pl
from jax.experimental.pallas import tpu as pltpu
from jax.sharding import PartitionSpec as P

ITERS = 2
EPS = 1e-06
GROUP = 2
COPY_TILES = 32
STEP_TILES = 64
VMEM_LIMIT = 28 * 1024 * 1024

F32 = jnp.float32
BF16 = jnp.bfloat16


def tile_sweep(
    live, chunk, group, count, pick, put, tiles, source, accum, before=None, beside=None
):
    zero_at = source.shape[0] - 1
    columns, edge = source.shape[1:]
    half = group // 2

    def one_group(base):
        blocks = []
        targets = []
        for t in range(group):
            at = base + t
            blocks.append(source[jnp.where(at < count, pick[at], zero_at)])
            targets.append(put[at])
        pad = jnp.zeros((columns * half, edge), F32)
        left = jnp.concatenate(
            [
                jnp.concatenate(blocks[0::2] + [pad], 0),
                jnp.concatenate([pad] + blocks[1::2], 0),
            ],
            1,
        ).astype(BF16)
        weights = [tiles[base + t] for t in range(group)]
        right = jnp.concatenate(
            [jnp.concatenate(weights[0::2], 1), jnp.concatenate(weights[1::2], 1)], 0
        )
        product = jnp.dot(left, right, preferred_element_type=F32)
        for t in range(group):
            first = (t % 2) * columns * half + (t // 2) * columns
            lane = (t // 2) * edge
            accum[targets[t]] += product[first : first + columns, lane : lane + edge]

    def one_chunk(c, carry):
        if before is not None:
            before(c)
        for g in range(chunk // group):
            one_group(c * chunk + g * group)
            if beside is not None:
                for t in range(group):
                    beside(c * chunk + g * group + t)
        return carry

    chunks = tiles.shape[0] // chunk

    if before is not None:
        lax.fori_loop(0, live, one_chunk, 0)
        return

    @pl.when(live == chunks)
    def _():
        for c in range(chunks):
            one_chunk(c, 0)

    @pl.when(live < chunks)
    def _():
        lax.fori_loop(0, live, one_chunk, 0)


def halving(bound):
    return 2.0 ** -max(0, math.ceil(math.log2(bound)) - 50)


def pack_blocks(accum, send, devices, slots_each):
    columns = accum.shape[1]
    for p in range(devices):
        both = jnp.concatenate([accum[p * slots_each + k] for k in range(slots_each)], 0)
        send[p, : slots_each * columns, :] = both.astype(BF16)


def solution(mesh):
    devices = mesh.shape["rows"]

    def per_device(edge_tiles, tile_row, tile_slot, tile_count, fetch_list, hub_start):
        tile_total, edge, _ = edge_tiles.shape
        columns = hub_start.shape[0]
        blocks = hub_start.shape[1] // edge
        slot_total = fetch_list.shape[1]
        slots_each = slot_total // devices
        node_total = hub_start.shape[1] * devices
        step = math.gcd(STEP_TILES, tile_total)
        chunk = math.gcd(COPY_TILES, step)
        group = math.gcd(GROUP, chunk)
        always = min(2, tile_total // chunk)
        rows_each = slots_each * columns
        rows_first = rows_each + slots_each + slots_each % 2
        assert group % 2 == 0

        by_column = 0.5 * tile_total * devices * edge
        by_row = 0.5 * tile_total * edge
        authority_bound = 6.0 * by_column * by_row * by_column
        authority_halving = halving(authority_bound)
        hub_halving = halving(authority_bound * by_row)

        smem = pl.BlockSpec(memory_space=pltpu.SMEM)
        vmem = pl.BlockSpec(memory_space=pltpu.VMEM)
        hbm = pl.BlockSpec(memory_space=pltpu.HBM)
        params = pltpu.CompilerParams(vmem_limit_bytes=VMEM_LIMIT)
        sweep_params = pltpu.CompilerParams(
            vmem_limit_bytes=VMEM_LIMIT
        )

        def start_kernel(
            cnt, row_hbm, slot_hbm, fetch_hbm, hub_hbm, tiles,
            send, kept, flipped, live_count, row_s, slot_s, fetch, hub, source, accum, sems, small
        ):
            def copy(c):
                span = pl.ds(c * chunk, chunk)
                return pltpu.make_async_copy(tiles.at[span], kept.at[span], sems.at[c])

            def begin(c, carry):
                copy(c).start()
                return carry

            def end(c, carry):
                copy(c).wait()
                return carry

            pairs = [(hub_hbm, hub), (row_hbm, row_s), (slot_hbm, slot_s), (fetch_hbm, fetch)]
            parts = [pltpu.make_async_copy(a, b, small.at[i]) for i, (a, b) in enumerate(pairs)]
            for part in parts:
                part.start()
            for c in range(always):
                copy(c).start()
            accum[...] = jnp.zeros_like(accum)
            source[blocks] = jnp.zeros((columns, edge), F32)
            count = cnt[0]
            live_count[...] = jnp.full(live_count.shape, count, jnp.int32)
            live = (count + step - 1) // step * (step // chunk)
            lax.fori_loop(always, live, begin, 0)
            for part in parts:
                part.wait()

            def flip(i):
                flipped[i] = kept[i].T

            for b in range(blocks):
                source[b] = hub[:, b * edge : (b + 1) * edge].astype(BF16).astype(F32)
            tile_sweep(
                live, chunk, group, count, row_s, slot_s, kept, source, accum,
                lambda c: copy(c).wait(), flip,
            )
            lax.fori_loop(live, always, end, 0)
            for p in range(devices):
                base = p * rows_first
                both = [accum[p * slots_each + k] for k in range(slots_each)]
                send[base : base + rows_each] = jnp.concatenate(both, 0).astype(BF16)
                wanted = [
                    jnp.full((1, edge), fetch[0, p * slots_each + k % slots_each], jnp.int32)
                    for k in range(rows_first - rows_each)
                ]
                send[base + rows_each : base + rows_first] = (
                    jnp.concatenate(wanted, 0).astype(F32).astype(BF16)
                )

        def sum_and_reply(got, base_rows, wanted, reply):
            totals = [jnp.zeros((columns, edge), F32) for _ in range(blocks)]
            for p in range(devices):
                base = p * base_rows
                values = got[base : base + rows_each].astype(F32)
                for k in range(slots_each):
                    value = values[k * columns : (k + 1) * columns]
                    block = wanted[p * slots_each + k]
                    for b in range(blocks):
                        totals[b] = totals[b] + jnp.where(block == b, value, 0.0)
            for p in range(devices):
                out = []
                for k in range(slots_each):
                    block = wanted[p * slots_each + k]
                    chosen = totals[0]
                    for b in range(1, blocks):
                        chosen = jnp.where(block == b, totals[b], chosen)
                    out.append(chosen)
                reply[p] = jnp.concatenate(out, 0).astype(BF16)
            return totals

        def first_owner_kernel(got, reply, wanted):
            for p in range(devices):
                base = p * rows_first
                rows = got[base + rows_each : base + rows_first].astype(F32)
                for k in range(slots_each):
                    wanted[p * slots_each + k] = jnp.broadcast_to(rows[k : k + 1], (columns, edge))
            sum_and_reply(got, rows_first, wanted, reply)

        def owner_kernel(got, wanted, reply, raw, squares):
            totals = sum_and_reply(got, rows_each, wanted, reply)
            square = jnp.zeros((columns, edge), F32)
            for b in range(blocks):
                raw[:, b * edge : (b + 1) * edge] = totals[b]
                scaled = totals[b] * authority_halving
                square = square + scaled * scaled
            squares[...] = square

        def load_fetched(fetched, source):
            for p in range(devices):
                both = fetched[p].astype(F32)
                for k in range(slots_each):
                    source[p * slots_each + k] = both[k * columns : (k + 1) * columns]
            source[slot_total] = jnp.zeros((columns, edge), F32)

        def begin_tables(*pairs_and_sems):
            *pairs, sems = pairs_and_sems
            copies = [pltpu.make_async_copy(a, b, sems.at[i]) for i, (a, b) in enumerate(pairs)]
            for each in copies:
                each.start()
            return copies

        def end_tables(copies, cnt):
            for each in copies:
                each.wait()
            return cnt[0, 0]

        def middle_kernel(
            cnt_v, row_v, slot_v, fetched, tiles, flipped,
            send, squares, source, hub, accum, low, cnt, row_s, slot_s, sems
        ):
            tables = begin_tables((cnt_v, cnt), (row_v, row_s), (slot_v, slot_s), sems)
            load_fetched(fetched, source)
            hub[...] = jnp.zeros_like(hub)
            accum[...] = jnp.zeros_like(accum)
            count = end_tables(tables, cnt)
            rounds = (count + step - 1) // step
            tile_sweep(rounds, step, group, count, slot_s, row_s, flipped, source, hub)
            square = jnp.zeros((columns, edge), F32)
            for b in range(blocks):
                value = hub[b]
                square = square + value * value
                low[b] = value.astype(BF16).astype(F32)
            low[blocks] = jnp.zeros((columns, edge), F32)
            squares[...] = square
            tile_sweep(rounds, step, group, count, row_s, slot_s, tiles, low, accum)
            pack_blocks(accum, send, devices, slots_each)

        def last_kernel(
            cnt_v, row_v, slot_v, fetched, flipped, first_squares, authority_squares,
            raw, send, source, hub, cnt, row_s, slot_s, sems
        ):
            tables = begin_tables((cnt_v, cnt), (row_v, row_s), (slot_v, slot_s), sems)
            load_fetched(fetched, source)
            hub[...] = jnp.zeros_like(hub)
            count = end_tables(tables, cnt)
            rounds = (count + step - 1) // step
            tile_sweep(rounds, step, group, count, slot_s, row_s, flipped, source, hub)
            square = jnp.zeros((columns, edge), F32)
            for b in range(blocks):
                value = hub[b]
                raw[:, b * edge : (b + 1) * edge] = value
                scaled = value * hub_halving
                square = square + scaled * scaled
            stats = [
                jnp.sum(first_squares[...], axis=1, keepdims=True),
                jnp.sum(authority_squares[...], axis=1, keepdims=True),
                jnp.sum(square, axis=1, keepdims=True),
            ]
            lane = lax.broadcasted_iota(jnp.int32, (columns, edge), 1)
            sub = lax.broadcasted_iota(jnp.int32, (columns, edge), 0)
            mixed = jnp.zeros((columns, edge), F32)
            for j, stat in enumerate(stats):
                mixed = jnp.where(lane == sub + j * columns, stat, mixed)
            line = jnp.sum(mixed, axis=0, keepdims=True)
            send[...] = jnp.broadcast_to(line, send.shape)

        def finish_kernel(got, hub_raw, authority_raw, hub, authority):
            sums = jnp.sum(got[...], axis=0, keepdims=True)
            lane = lax.broadcasted_iota(jnp.int32, (columns, edge), 1)
            sub = lax.broadcasted_iota(jnp.int32, (columns, edge), 0)

            def mean(j):
                spread = jnp.broadcast_to(sums, (columns, edge))
                kept = jnp.where(lane == sub + j * columns, spread, 0.0)
                return jnp.sum(kept, axis=1, keepdims=True) * (1.0 / node_total)

            first = mean(0) + EPS

            def factor(j, half):
                return half / jnp.sqrt(mean(j) + (half * half * EPS) * first)

            authority[...] = authority_raw[...] * factor(1, authority_halving)
            hub[...] = hub_raw[...] * factor(2, hub_halving)

        def shape(dims, kind):
            return jax.ShapeDtypeStruct(dims, kind)

        block_shape = (columns, edge)
        source_blocks = pltpu.VMEM((blocks + 1,) + block_shape, F32)
        source_slots = pltpu.VMEM((slot_total + 1,) + block_shape, F32)
        sum_blocks = pltpu.VMEM((blocks,) + block_shape, F32)
        sum_slots = pltpu.VMEM((slot_total,) + block_shape, F32)
        whole = shape((columns, blocks * edge), F32)
        plain = shape((devices, rows_each, edge), BF16)
        square_shape = shape(block_shape, F32)

        def exchange(value):
            return lax.all_to_all(value, "rows", split_axis=0, concat_axis=0, tiled=True)

        small = [tile_count, tile_row, tile_slot]
        operands = small + [fetch_list, hub_start, edge_tiles]
        send, tiles, flipped, live_count = pl.pallas_call(
            start_kernel,
            name="start",
            out_shape=(
                shape((devices * rows_first, edge), BF16),
                shape(edge_tiles.shape, edge_tiles.dtype),
                shape(edge_tiles.shape, edge_tiles.dtype),
                shape((1, edge), jnp.int32),
            ),
            in_specs=[smem] + [hbm] * 5,
            out_specs=(vmem,) * 4,
            scratch_shapes=[
                *[pltpu.SMEM(a.shape, a.dtype) for a in small[1:]],
                pltpu.SMEM(fetch_list.shape, fetch_list.dtype),
                pltpu.VMEM(hub_start.shape, F32),
                source_blocks,
                sum_slots,
                pltpu.SemaphoreType.DMA((tile_total // chunk,)),
                pltpu.SemaphoreType.DMA((4,)),
            ],
            compiler_params=params,
        )(tile_count, *[pltpu.with_memory_space_constraint(a, pltpu.HBM) for a in operands[1:]])
        halves = (devices, rows_first // 2, 2, edge)
        first = exchange(send.reshape(halves)).reshape(send.shape)
        small = [live_count, tile_row, tile_slot]
        table_scratch = [pltpu.SMEM(a.shape, a.dtype) for a in small]
        table_scratch.append(pltpu.SemaphoreType.DMA((len(small),)))

        reply, wanted = pl.pallas_call(
            first_owner_kernel,
            name="first_owner",
            out_shape=(plain, shape((slot_total,) + block_shape, F32)),
            in_specs=[vmem],
            out_specs=(vmem, vmem),
            compiler_params=params,
        )(first)
        send, first_squares = pl.pallas_call(
            middle_kernel,
            name="middle",
            out_shape=(plain, square_shape),
            in_specs=[vmem] * 6,
            out_specs=(vmem, vmem),
            scratch_shapes=[source_slots, sum_blocks, sum_slots, source_blocks, *table_scratch],
            compiler_params=sweep_params,
        )(*small, exchange(reply), tiles, flipped)
        reply, authority_raw, authority_squares = pl.pallas_call(
            owner_kernel,
            name="owner",
            out_shape=(plain, whole, square_shape),
            in_specs=[vmem, vmem],
            out_specs=(vmem, vmem, vmem),
            compiler_params=params,
        )(exchange(send).reshape(devices * rows_each, edge), wanted)
        hub_raw, send = pl.pallas_call(
            last_kernel,
            name="last",
            out_shape=(whole, shape((devices, edge), F32)),
            in_specs=[vmem] * 7,
            out_specs=(vmem, vmem),
            scratch_shapes=[source_slots, sum_blocks, *table_scratch],
            compiler_params=sweep_params,
        )(*small, exchange(reply), flipped, first_squares, authority_squares)
        return pl.pallas_call(
            finish_kernel,
            name="finish",
            out_shape=(whole, whole),
            in_specs=[vmem, vmem, vmem],
            out_specs=(vmem, vmem),
            compiler_params=params,
        )(exchange(send), hub_raw, authority_raw)

    in_specs = (
        P("rows", None, None),
        P("rows"),
        P("rows"),
        P("rows"),
        P("rows", None),
        P(None, "rows"),
    )
    out_specs = (P(None, "rows"), P(None, "rows"))
    return jax.shard_map(
        per_device, mesh=mesh, in_specs=in_specs, out_specs=out_specs, check_vma=False
    )
```

```python
import math

import jax
import jax.numpy as jnp
from jax import lax
from jax.experimental import pallas as pl
from jax.experimental.pallas import tpu as pltpu
from jax.sharding import PartitionSpec as P

ITERS = 2
EPS = 1e-06
GROUP = 2
COPY_TILES = 32
STEP_TILES = 64
VMEM_LIMIT = 28 * 1024 * 1024

F32 = jnp.float32
BF16 = jnp.bfloat16


def tile_sweep(
    live, chunk, group, count, pick, put, tiles, source, accum, before=None, beside=None
):
    zero_at = source.shape[0] - 1
    columns, edge = source.shape[1:]
    half = group // 2

    def one_group(base):
        blocks = []
        targets = []
        for t in range(group):
            at = base + t
            blocks.append(source[jnp.where(at < count, pick[at], zero_at)])
            targets.append(put[at])
        pad = jnp.zeros((columns * half, edge), F32)
        left = jnp.concatenate(
            [
                jnp.concatenate(blocks[0::2] + [pad], 0),
                jnp.concatenate([pad] + blocks[1::2], 0),
            ],
            1,
        ).astype(BF16)
        weights = [tiles[base + t] for t in range(group)]
        right = jnp.concatenate(
            [jnp.concatenate(weights[0::2], 1), jnp.concatenate(weights[1::2], 1)], 0
        )
        product = jnp.dot(left, right, preferred_element_type=F32)
        for t in range(group):
            first = (t % 2) * columns * half + (t // 2) * columns
            lane = (t // 2) * edge
            accum[targets[t]] += product[first : first + columns, lane : lane + edge]

    def one_chunk(c, carry):
        if before is not None:
            before(c)
        for g in range(chunk // group):
            one_group(c * chunk + g * group)
            if beside is not None:
                for t in range(group):
                    beside(c * chunk + g * group + t)
        return carry

    chunks = tiles.shape[0] // chunk

    if before is not None:
        lax.fori_loop(0, live, one_chunk, 0)
        return

    @pl.when(live == chunks)
    def _():
        for c in range(chunks):
            one_chunk(c, 0)

    @pl.when(live < chunks)
    def _():
        lax.fori_loop(0, live, one_chunk, 0)


def halving(bound):
    return 2.0 ** -max(0, math.ceil(math.log2(bound)) - 50)


def pack_blocks(accum, send, devices, slots_each):
    columns = accum.shape[1]
    for p in range(devices):
        both = jnp.concatenate([accum[p * slots_each + k] for k in range(slots_each)], 0)
        send[p, : slots_each * columns, :] = both.astype(BF16)


def solution(mesh):
    devices = mesh.shape["rows"]

    def per_device(edge_tiles, tile_row, tile_slot, tile_count, fetch_list, hub_start):
        tile_total, edge, _ = edge_tiles.shape
        columns = hub_start.shape[0]
        blocks = hub_start.shape[1] // edge
        slot_total = fetch_list.shape[1]
        slots_each = slot_total // devices
        node_total = hub_start.shape[1] * devices
        step = math.gcd(STEP_TILES, tile_total)
        chunk = math.gcd(COPY_TILES, step)
        group = math.gcd(GROUP, chunk)
        always = min(2, tile_total // chunk)
        rows_each = slots_each * columns
        rows_first = rows_each + slots_each + slots_each % 2
        assert group % 2 == 0

        by_column = 0.5 * tile_total * devices * edge
        by_row = 0.5 * tile_total * edge
        authority_bound = 6.0 * by_column * by_row * by_column
        authority_halving = halving(authority_bound)
        hub_halving = halving(authority_bound * by_row)

        smem = pl.BlockSpec(memory_space=pltpu.SMEM)
        vmem = pl.BlockSpec(memory_space=pltpu.VMEM)
        hbm = pl.BlockSpec(memory_space=pltpu.HBM)
        params = pltpu.CompilerParams(vmem_limit_bytes=VMEM_LIMIT)
        sweep_params = pltpu.CompilerParams(
            vmem_limit_bytes=VMEM_LIMIT
        )

        def start_kernel(
            cnt, row_hbm, slot_hbm, fetch_hbm, hub_hbm, tiles,
            send, kept, flipped, live_count, row_s, slot_s, fetch, hub, source, accum, sems, small
        ):
            def copy(c):
                span = pl.ds(c * chunk, chunk)
                return pltpu.make_async_copy(tiles.at[span], kept.at[span], sems.at[c])

            def begin(c, carry):
                copy(c).start()
                return carry

            def end(c, carry):
                copy(c).wait()
                return carry

            pairs = [(hub_hbm, hub), (row_hbm, row_s), (slot_hbm, slot_s), (fetch_hbm, fetch)]
            parts = [pltpu.make_async_copy(a, b, small.at[i]) for i, (a, b) in enumerate(pairs)]
            for part in parts:
                part.start()
            for c in range(always):
                copy(c).start()
            accum[...] = jnp.zeros_like(accum)
            source[blocks] = jnp.zeros((columns, edge), F32)
            count = cnt[0]
            live_count[...] = jnp.full(live_count.shape, count, jnp.int32)
            live = (count + step - 1) // step * (step // chunk)
            lax.fori_loop(always, live, begin, 0)
            for part in parts:
                part.wait()

            def flip(i):
                flipped[i] = kept[i].T

            for b in range(blocks):
                source[b] = hub[:, b * edge : (b + 1) * edge].astype(BF16).astype(F32)
            for p in range(devices):
                base = p * rows_first
                wanted = [
                    jnp.full((1, edge), fetch[0, p * slots_each + k % slots_each], jnp.int32)
                    for k in range(rows_first - rows_each)
                ]
                send[base + rows_each : base + rows_first] = (
                    jnp.concatenate(wanted, 0).astype(F32).astype(BF16)
                )
            tile_sweep(
                live, chunk, group, count, row_s, slot_s, kept, source, accum,
                lambda c: copy(c).wait(), flip,
            )
            lax.fori_loop(live, always, end, 0)
            for p in range(devices):
                base = p * rows_first
                both = [accum[p * slots_each + k] for k in range(slots_each)]
                send[base : base + rows_each] = jnp.concatenate(both, 0).astype(BF16)

        def sum_and_reply(got, base_rows, wanted, reply):
            totals = [jnp.zeros((columns, edge), F32) for _ in range(blocks)]
            for p in range(devices):
                base = p * base_rows
                values = got[base : base + rows_each].astype(F32)
                for k in range(slots_each):
                    value = values[k * columns : (k + 1) * columns]
                    block = wanted[p * slots_each + k]
                    for b in range(blocks):
                        totals[b] = totals[b] + jnp.where(block == b, value, 0.0)
            for p in range(devices):
                out = []
                for k in range(slots_each):
                    block = wanted[p * slots_each + k]
                    chosen = totals[0]
                    for b in range(1, blocks):
                        chosen = jnp.where(block == b, totals[b], chosen)
                    out.append(chosen)
                reply[p] = jnp.concatenate(out, 0).astype(BF16)
            return totals

        def first_owner_kernel(got, reply, wanted):
            for p in range(devices):
                base = p * rows_first
                rows = got[base + rows_each : base + rows_first].astype(F32)
                for k in range(slots_each):
                    wanted[p * slots_each + k] = jnp.broadcast_to(rows[k : k + 1], (columns, edge))
            sum_and_reply(got, rows_first, wanted, reply)

        def owner_kernel(got, wanted, reply, raw, squares):
            totals = sum_and_reply(got, rows_each, wanted, reply)
            square = jnp.zeros((columns, edge), F32)
            for b in range(blocks):
                raw[:, b * edge : (b + 1) * edge] = totals[b]
                scaled = totals[b] * authority_halving
                square = square + scaled * scaled
            squares[...] = square

        def load_fetched(fetched, source):
            for p in range(devices):
                both = fetched[p].astype(F32)
                for k in range(slots_each):
                    source[p * slots_each + k] = both[k * columns : (k + 1) * columns]
            source[slot_total] = jnp.zeros((columns, edge), F32)

        def begin_tables(*pairs_and_sems):
            *pairs, sems = pairs_and_sems
            copies = [pltpu.make_async_copy(a, b, sems.at[i]) for i, (a, b) in enumerate(pairs)]
            for each in copies:
                each.start()
            return copies

        def end_tables(copies, cnt):
            for each in copies:
                each.wait()
            return cnt[0, 0]

        def middle_kernel(
            cnt_v, row_v, slot_v, fetched, tiles, flipped,
            send, squares, source, hub, accum, low, cnt, row_s, slot_s, sems
        ):
            tables = begin_tables((cnt_v, cnt), (row_v, row_s), (slot_v, slot_s), sems)
            load_fetched(fetched, source)
            hub[...] = jnp.zeros_like(hub)
            accum[...] = jnp.zeros_like(accum)
            count = end_tables(tables, cnt)
            rounds = (count + step - 1) // step
            tile_sweep(rounds, step, group, count, slot_s, row_s, flipped, source, hub)
            square = jnp.zeros((columns, edge), F32)
            for b in range(blocks):
                value = hub[b]
                square = square + value * value
                low[b] = value.astype(BF16).astype(F32)
            low[blocks] = jnp.zeros((columns, edge), F32)
            squares[...] = square
            tile_sweep(rounds, step, group, count, row_s, slot_s, tiles, low, accum)
            pack_blocks(accum, send, devices, slots_each)

        def last_kernel(
            cnt_v, row_v, slot_v, fetched, flipped, first_squares, authority_squares,
            raw, send, source, hub, cnt, row_s, slot_s, sems
        ):
            tables = begin_tables((cnt_v, cnt), (row_v, row_s), (slot_v, slot_s), sems)
            load_fetched(fetched, source)
            hub[...] = jnp.zeros_like(hub)
            lane = lax.broadcasted_iota(jnp.int32, (columns, edge), 1)
            sub = lax.broadcasted_iota(jnp.int32, (columns, edge), 0)

            def place(mixed, j, squares):
                total = jnp.sum(squares, axis=1, keepdims=True)
                return jnp.where(lane == sub + j * columns, total, mixed)

            mixed = place(jnp.zeros((columns, edge), F32), 0, first_squares[...])
            mixed = place(mixed, 1, authority_squares[...])
            count = end_tables(tables, cnt)
            rounds = (count + step - 1) // step
            tile_sweep(rounds, step, group, count, slot_s, row_s, flipped, source, hub)
            square = jnp.zeros((columns, edge), F32)
            for b in range(blocks):
                value = hub[b]
                raw[:, b * edge : (b + 1) * edge] = value
                scaled = value * hub_halving
                square = square + scaled * scaled
            mixed = place(mixed, 2, square)
            line = jnp.sum(mixed, axis=0, keepdims=True)
            send[...] = jnp.broadcast_to(line, send.shape)

        def finish_kernel(
            got, hub_raw, authority_raw, hub_hbm, authority_hbm, hub, authority, sems
        ):
            sums = jnp.sum(got[...], axis=0, keepdims=True)
            lane = lax.broadcasted_iota(jnp.int32, (columns, edge), 1)
            sub = lax.broadcasted_iota(jnp.int32, (columns, edge), 0)

            def mean(j):
                spread = jnp.broadcast_to(sums, (columns, edge))
                kept = jnp.where(lane == sub + j * columns, spread, 0.0)
                return jnp.sum(kept, axis=1, keepdims=True) * (1.0 / node_total)

            first = mean(0) + EPS

            def factor(j, half):
                return half / jnp.sqrt(mean(j) + (half * half * EPS) * first)

            authority[...] = authority_raw[...] * factor(1, authority_halving)
            copies = [
                pltpu.make_async_copy(authority, authority_hbm, sems.at[0]),
                pltpu.make_async_copy(hub, hub_hbm, sems.at[1]),
            ]
            copies[0].start()
            hub[...] = hub_raw[...] * factor(2, hub_halving)
            copies[1].start()
            for each in copies:
                each.wait()

        def shape(dims, kind):
            return jax.ShapeDtypeStruct(dims, kind)

        block_shape = (columns, edge)
        source_blocks = pltpu.VMEM((blocks + 1,) + block_shape, F32)
        source_slots = pltpu.VMEM((slot_total + 1,) + block_shape, F32)
        sum_blocks = pltpu.VMEM((blocks,) + block_shape, F32)
        sum_slots = pltpu.VMEM((slot_total,) + block_shape, F32)
        whole = shape((columns, blocks * edge), F32)
        plain = shape((devices, rows_each, edge), BF16)
        square_shape = shape(block_shape, F32)

        def exchange(value):
            return lax.all_to_all(value, "rows", split_axis=0, concat_axis=0, tiled=True)

        small = [tile_count, tile_row, tile_slot]
        operands = small + [fetch_list, hub_start, edge_tiles]
        send, tiles, flipped, live_count = pl.pallas_call(
            start_kernel,
            name="start",
            out_shape=(
                shape((devices * rows_first, edge), BF16),
                shape(edge_tiles.shape, edge_tiles.dtype),
                shape(edge_tiles.shape, edge_tiles.dtype),
                shape((1, edge), jnp.int32),
            ),
            in_specs=[smem] + [hbm] * 5,
            out_specs=(vmem,) * 4,
            scratch_shapes=[
                *[pltpu.SMEM(a.shape, a.dtype) for a in small[1:]],
                pltpu.SMEM(fetch_list.shape, fetch_list.dtype),
                pltpu.VMEM(hub_start.shape, F32),
                source_blocks,
                sum_slots,
                pltpu.SemaphoreType.DMA((tile_total // chunk,)),
                pltpu.SemaphoreType.DMA((4,)),
            ],
            compiler_params=params,
        )(tile_count, *[pltpu.with_memory_space_constraint(a, pltpu.HBM) for a in operands[1:]])
        halves = (devices, rows_first // 2, 2, edge)
        first = exchange(send.reshape(halves)).reshape(send.shape)
        small = [live_count, tile_row, tile_slot]
        table_scratch = [pltpu.SMEM(a.shape, a.dtype) for a in small]
        table_scratch.append(pltpu.SemaphoreType.DMA((len(small),)))

        reply, wanted = pl.pallas_call(
            first_owner_kernel,
            name="first_owner",
            out_shape=(plain, shape((slot_total,) + block_shape, F32)),
            in_specs=[vmem],
            out_specs=(vmem, vmem),
            compiler_params=params,
        )(first)
        send, first_squares = pl.pallas_call(
            middle_kernel,
            name="middle",
            out_shape=(plain, square_shape),
            in_specs=[vmem] * 6,
            out_specs=(vmem, vmem),
            scratch_shapes=[source_slots, sum_blocks, sum_slots, source_blocks, *table_scratch],
            compiler_params=sweep_params,
        )(*small, exchange(reply), tiles, flipped)
        reply, authority_raw, authority_squares = pl.pallas_call(
            owner_kernel,
            name="owner",
            out_shape=(plain, whole, square_shape),
            in_specs=[vmem, vmem],
            out_specs=(vmem, vmem, vmem),
            compiler_params=params,
        )(exchange(send).reshape(devices * rows_each, edge), wanted)
        hub_raw, send = pl.pallas_call(
            last_kernel,
            name="last",
            out_shape=(whole, shape((devices, edge), F32)),
            in_specs=[vmem] * 7,
            out_specs=(vmem, vmem),
            scratch_shapes=[source_slots, sum_blocks, *table_scratch],
            compiler_params=sweep_params,
        )(*small, exchange(reply), flipped, first_squares, authority_squares)
        return pl.pallas_call(
            finish_kernel,
            name="finish",
            out_shape=(whole, whole),
            in_specs=[vmem, vmem, vmem],
            out_specs=(hbm, hbm),
            scratch_shapes=[
                pltpu.VMEM(whole.shape, F32),
                pltpu.VMEM(whole.shape, F32),
                pltpu.SemaphoreType.DMA((2,)),
            ],
            compiler_params=params,
        )(exchange(send), hub_raw, authority_raw)

    in_specs = (
        P("rows", None, None),
        P("rows"),
        P("rows"),
        P("rows"),
        P("rows", None),
        P(None, "rows"),
    )
    out_specs = (P(None, "rows"), P(None, "rows"))
    return jax.shard_map(
        per_device, mesh=mesh, in_specs=in_specs, out_specs=out_specs, check_vma=False
    )
```
